32 devices in a mesh: row: 4 (over y, core), col: 8 (over z, x).
Axes of the slice: x: 2, y: 2, z: 4, core: 2. Of those that a mesh axis runs over, the one named last changes fastest.
Arguments:
- start_field: float32 [1, 2, 4096, 8192], P(None, None, 'col', 'row'), may hold values from -6 to 6
- section_field: float32 [1, 2, 4096, 8192], P(None, None, 'col', 'row'), may hold values from -26 to 26
- start_term: float32 [1, 2, 4096, 8192], P(None, None, 'col', 'row'), may hold values from -6 to 6
- first_term: float32 [1, 2, 4096, 8192], P(None, None, 'col', 'row'), may hold values from -6 to 6
- second_term: float32 [1, 2, 4096, 8192], P(None, None, 'col', 'row'), may hold values from -6 to 6
Outputs:
- next_field: float32 [1, 2, 4096, 8192], P(None, None, 'col', 'row')
The draws below stay inside these ranges and needn't reach their ends.
All inputs are finite; a program needn't handle non-finite values.
Results may differ from the reference program's by a relative error of at most 0.0001.
Values sent between devices are 32-bit elements; how exact they have to be, the bound alone decides.
A program may use at most 256 MiB of HBM per device.

```python
import math
import jax
import jax.numpy as jnp
from jax import lax

N = 8192
MEMBERS = 1
NK = 4096


def draw_section_field(key, part):
    wave_x = lax.broadcasted_iota(jnp.int32, (NK, N), 0)
    index_y = lax.broadcasted_iota(jnp.int32, (NK, N), 1)
    wave_y = jnp.where(index_y < N // 2, index_y, index_y - N)
    envelope = 3.0 * jnp.sqrt((wave_x * wave_x + wave_y * wave_y).astype(jnp.float32)) / N
    noise = jnp.clip(jax.random.normal(key, (MEMBERS, 2, NK, N), jnp.float32), -6.0, 6.0)
    return 2.0 * envelope * noise


def steps_of(key, dims, split, smallest, largest):
    factor_of, own = 1.0, jax.random.fold_in(key, 6)
    for dim, blocks in split:
        steps = jnp.exp(jax.random.uniform(jax.random.fold_in(own, dim), (blocks,), jnp.float32, smallest / len(split), largest / len(split)))
        factor_of = factor_of * jnp.repeat(steps, dims[dim] // blocks).reshape([-1 if axis == dim else 1 for axis in range(len(dims))])
    return factor_of


def gaussian(key, extent, deviation, limit, cuts=(), dtype=jnp.bfloat16):
    drawn = deviation * jax.random.normal(key, extent, jnp.float32)
    if cuts:
        drawn = drawn * steps_of(key, extent, cuts, -0.22, 0.18)
    return jnp.clip(drawn, -limit, limit).astype(dtype)


def setup_inputs(seed: int = 0) -> dict:
    seeds = jax.random.split(jax.random.key(seed), 6)
    start_field = gaussian(seeds[0], (MEMBERS, 2, NK, N), 1.0, 6.0, ((2, 8), (3, 4)), jnp.float32)
    section_field = draw_section_field(jax.random.fold_in(seeds[5], 71), 0)
    start_term = gaussian(seeds[2], (MEMBERS, 2, NK, N), 1.0, 6.0, ((2, 8), (3, 4)), jnp.float32)
    first_term = gaussian(seeds[3], (MEMBERS, 2, NK, N), 1.0, 6.0, ((2, 8), (3, 4)), jnp.float32)
    second_term = gaussian(seeds[4], (MEMBERS, 2, NK, N), 1.0, 6.0, ((2, 8), (3, 4)), jnp.float32)
    return dict(start_field=start_field, section_field=section_field, start_term=start_term, first_term=first_term, second_term=second_term)


viscous_rate = 1.5
wave_scale = 3.0
series_terms = 12


def section_weights(wave_x, wave_y, length):
    square = wave_x * wave_x + wave_y * wave_y
    kappa_x = wave_scale * wave_x.astype(jnp.float32) / length
    kappa_y = wave_scale * wave_y.astype(jnp.float32) / length
    kappa_sq = kappa_x * kappa_x + kappa_y * kappa_y
    zvalue = -viscous_rate * kappa_sq
    damping = jnp.exp(zvalue)
    near_zero = 27 * square < 2 * length * length

    def series(degree):
        running = jnp.full_like(zvalue, 1.0 / math.factorial(series_terms - 1 + degree))
        for term_index in range(series_terms - 2, -1, -1):
            running = running * zvalue + 1.0 / math.factorial(term_index + degree)
        return running

    clamped = jnp.where(near_zero, -1.0, zvalue)
    exp_clamped = jnp.exp(clamped)
    closed_one = (exp_clamped - 1.0) / clamped
    closed_two = (exp_clamped - 1.0 - clamped) / (clamped * clamped)
    closed_three = (exp_clamped - 1.0 - clamped - 0.5 * clamped * clamped) / (clamped * clamped * clamped)
    phi_one = jnp.where(near_zero, series(1), closed_one)
    phi_two = jnp.where(near_zero, series(2), closed_two)
    phi_three = jnp.where(near_zero, series(3), closed_three)
    weight_a = phi_one - 3.0 * phi_two + 4.0 * phi_three
    weight_b = phi_two - 2.0 * phi_three
    weight_c = 4.0 * phi_three - phi_two
    keep_mask = ((3 * jnp.abs(wave_x) < length) & (3 * jnp.abs(wave_y) < length)).astype(jnp.float32)
    inverse_sq = (length * length) / (9.0 * jnp.maximum(square, 1).astype(jnp.float32))
    return damping, weight_a, weight_b, weight_c, kappa_x, kappa_y, keep_mask, inverse_sq


def to_grid(real_part, imag_part):
    length = real_part.shape[1]
    complex_spec = lax.complex(real_part, imag_part)
    along_y = jnp.fft.ifft(complex_spec, axis=1)
    return jnp.fft.irfft(along_y, n=length, axis=0) * length


def to_spectrum(real_grid):
    length = real_grid.shape[0]
    along_x = jnp.fft.rfft(real_grid, axis=0)[: length // 2]
    spectrum = jnp.fft.fft(along_x, axis=1) / length
    return jnp.real(spectrum), jnp.imag(spectrum)


def reference(start_field, section_field, start_term, first_term, second_term):
    length = start_field.shape[3]
    wave_x = lax.broadcasted_iota(jnp.int32, (length // 2, length), 0)
    index_y = lax.broadcasted_iota(jnp.int32, (length // 2, length), 1)
    wave_y = jnp.where(index_y < length // 2, index_y, index_y - length)
    damping, weight_a, weight_b, weight_c, kappa_x, kappa_y, keep_mask, inverse_sq = section_weights(wave_x, wave_y, length)
    section_terms = []
    for member in range(section_field.shape[0]):
        real_part = section_field[member, 0] * keep_mask
        imag_part = section_field[member, 1] * keep_mask
        psi_real = real_part * inverse_sq
        psi_imag = imag_part * inverse_sq
        vel_u = to_grid(-kappa_y * psi_imag, kappa_y * psi_real)
        grad_x = to_grid(-kappa_x * imag_part, kappa_x * real_part)
        jacobian = vel_u * grad_x
        vel_v = to_grid(kappa_x * psi_imag, -kappa_x * psi_real)
        grad_y = to_grid(-kappa_y * imag_part, kappa_y * real_part)
        jacobian = jacobian + vel_v * grad_y
        jac_real, jac_imag = to_spectrum(jacobian)
        section_terms.append(jnp.stack([-keep_mask * jac_real, -keep_mask * jac_imag]))
    section_term = jnp.stack(section_terms)
    return damping * start_field + weight_a * start_term + 2.0 * weight_b * (first_term + second_term) + weight_c * section_term
```

```python
import math

import jax
import jax.numpy as jnp
from jax import lax
from jax.sharding import PartitionSpec as P

RADIX = 128


viscous_rate = 1.5
wave_scale = 3.0
series_terms = 12


def section_weights(wave_x, wave_y, length):
    square = wave_x * wave_x + wave_y * wave_y
    kappa_x = wave_scale * wave_x.astype(jnp.float32) / length
    kappa_y = wave_scale * wave_y.astype(jnp.float32) / length
    kappa_sq = kappa_x * kappa_x + kappa_y * kappa_y
    zvalue = -viscous_rate * kappa_sq
    damping = jnp.exp(zvalue)
    near_zero = 27 * square < 2 * length * length

    def series(degree):
        running = jnp.full_like(zvalue, 1.0 / math.factorial(series_terms - 1 + degree))
        for term_index in range(series_terms - 2, -1, -1):
            running = running * zvalue + 1.0 / math.factorial(term_index + degree)
        return running

    clamped = jnp.where(near_zero, -1.0, zvalue)
    exp_clamped = jnp.exp(clamped)
    closed_one = (exp_clamped - 1.0) / clamped
    closed_two = (exp_clamped - 1.0 - clamped) / (clamped * clamped)
    closed_three = (exp_clamped - 1.0 - clamped - 0.5 * clamped * clamped) / (
        clamped * clamped * clamped
    )
    phi_one = jnp.where(near_zero, series(1), closed_one)
    phi_two = jnp.where(near_zero, series(2), closed_two)
    phi_three = jnp.where(near_zero, series(3), closed_three)
    weight_a = phi_one - 3.0 * phi_two + 4.0 * phi_three
    weight_b = phi_two - 2.0 * phi_three
    weight_c = 4.0 * phi_three - phi_two
    keep_mask = ((3 * jnp.abs(wave_x) < length) & (3 * jnp.abs(wave_y) < length)).astype(
        jnp.float32
    )
    inverse_sq = length * length / (9.0 * jnp.maximum(square, 1).astype(jnp.float32))
    return (damping, weight_a, weight_b, weight_c, kappa_x, kappa_y, keep_mask, inverse_sq)


def section_table(count_in, count_out, period, direction):
    row_ids = lax.broadcasted_iota(jnp.int32, (count_in, count_out), 0)
    col_ids = lax.broadcasted_iota(jnp.int32, (count_in, count_out), 1)
    angles = direction * 2.0 * math.pi / period * (row_ids * col_ids % period).astype(jnp.float32)
    cosine = jnp.cos(angles)
    sine_part = jnp.sin(angles)
    return jnp.stack(
        [jnp.stack([cosine, sine_part], axis=1), jnp.stack([-sine_part, cosine], axis=1)], axis=0
    )


def twiddle(count_c, count_b, period, direction):
    row_ids = lax.broadcasted_iota(jnp.int32, (count_c, count_b), 0)
    col_ids = lax.broadcasted_iota(jnp.int32, (count_c, count_b), 1)
    angles = direction * 2.0 * math.pi / period * (row_ids * col_ids % period).astype(jnp.float32)
    return (jnp.cos(angles), jnp.sin(angles))


def rotate(values, cosine, sine_part):
    return jnp.stack(
        [values[0] * cosine - values[1] * sine_part, values[0] * sine_part + values[1] * cosine]
    )


def product(equation, left, right):
    return jnp.einsum(equation, left, right, precision=lax.Precision.HIGH)


def lines_inverse(pieces):
    parts, count_k, length = pieces.shape
    count_b = RADIX
    count_a = length // count_b
    shaped = pieces.reshape((parts, count_k, count_a, count_b))
    first = product("pkab,pasc->skcb", shaped, section_table(count_a, count_a, count_a, 1.0))
    first = rotate(first, *twiddle(count_a, count_b, length, 1.0))
    second = product("pkcb,pbsd->skcd", first, section_table(count_b, count_b, count_b, 1.0))
    return second.reshape((parts, count_k, length))


def lines_forward(pieces):
    parts, count_k, length = pieces.shape
    count_d = RADIX
    count_c = length // count_d
    shaped = pieces.reshape((parts, count_k, count_c, count_d))
    first = product("pkcd,pdsf->skcf", shaped, section_table(count_d, count_d, count_d, -1.0))
    first = rotate(first, *twiddle(count_c, count_d, length, -1.0))
    second = product("pkcf,pcse->skef", first, section_table(count_c, count_c, count_c, -1.0))
    return second.reshape((parts, count_k, length))


def turned_table(count_c, count_b, period, direction):
    c_ids = lax.broadcasted_iota(jnp.int32, (count_c, count_b, count_b), 0)
    b_ids = lax.broadcasted_iota(jnp.int32, (count_c, count_b, count_b), 1)
    d_ids = lax.broadcasted_iota(jnp.int32, (count_c, count_b, count_b), 2)
    steps = b_ids * (c_ids + count_c * d_ids) % period
    angles = direction * 2.0 * math.pi / period * steps.astype(jnp.float32)
    return jnp.cos(angles), jnp.sin(angles)


def columns_inverse(pieces, table):
    parts, half_count, count_y = pieces.shape
    count_a = half_count // RADIX
    count_c = 2 * count_a
    shaped = pieces.reshape((parts, count_a, RADIX, count_y))
    first = product("paby,pasc->csby", shaped, section_table(count_a, count_c, count_c, 1.0))
    return product("csby,csbd->cdy", first, table)


def columns_forward(grid, table):
    count_c, count_d, count_y = grid.shape
    half_count = count_c // 2
    first = product("cdy,cpfd->cpfy", grid, table)
    second = product(
        "cpfy,pcse->sefy", first, section_table(count_c, half_count, count_c, -1.0)
    )
    return second.reshape((2, half_count * count_d, count_y))


def to_columns(lines):
    return lax.all_to_all(lines, ("col", "row"), split_axis=2, concat_axis=1, tiled=True)


def to_lines(columns):
    return lax.all_to_all(columns, ("col", "row"), split_axis=1, concat_axis=2, tiled=True)


def positions(shape, start_x, start_y, length):
    wave_x = start_x + lax.broadcasted_iota(jnp.int32, shape, 0)
    index_y = start_y + lax.broadcasted_iota(jnp.int32, shape, 1)
    wave_y = jnp.where(index_y < length // 2, index_y, index_y - length)
    return wave_x, wave_y


def nonlinear(section_field, length):
    block_x = section_field.shape[1]
    lines = lax.all_to_all(section_field, "row", split_axis=1, concat_axis=2, tiled=True)
    count_k = lines.shape[1]
    start_x = lax.axis_index("col") * block_x + lax.axis_index("row") * count_k
    wave_x, wave_y = positions((count_k, length), start_x, 0, length)
    square = wave_x * wave_x + wave_y * wave_y
    kappa_x = wave_scale * wave_x.astype(jnp.float32) / length
    kappa_y = wave_scale * wave_y.astype(jnp.float32) / length
    keep = (3 * jnp.abs(wave_x) < length) & (3 * jnp.abs(wave_y) < length)
    doubled = jnp.where(wave_x == 0, 1.0, 2.0) * (1.0 / length)
    inverse_sq = length * length / (9.0 * jnp.maximum(square, 1).astype(jnp.float32))
    factor = jnp.where(keep, inverse_sq * doubled, 0.0)
    scale_u = kappa_y * factor
    scale_v = kappa_x * factor
    spec_u = jnp.stack([-scale_u * lines[1], scale_u * lines[0]])
    spec_v = jnp.stack([scale_v * lines[1], -scale_v * lines[0]])
    count_c = length // RADIX
    cosine, sine_part = turned_table(count_c, RADIX, length, 1.0)
    table = jnp.stack([cosine, -sine_part], axis=1)
    vel_u = columns_inverse(to_columns(lines_inverse(spec_u)), table)
    vel_v = columns_inverse(to_columns(lines_inverse(spec_v)), table)
    cross = lines_forward(to_lines(columns_forward(vel_u * vel_v, table)))
    square_gap = lines_forward(
        to_lines(columns_forward((vel_v - vel_u) * (vel_v + vel_u), table))
    )
    scale = jnp.where(keep, 1.0 / length, 0.0)
    weight_cross = (kappa_x * kappa_x - kappa_y * kappa_y) * scale
    weight_gap = kappa_x * kappa_y * scale
    term = weight_cross * cross + weight_gap * square_gap
    return lax.all_to_all(term, "row", split_axis=2, concat_axis=1, tiled=True)


def per_device(start_field, section_field, start_term, first_term, second_term):
    members = start_field.shape[0]
    block_x = start_field.shape[2]
    block_y = start_field.shape[3]
    length = block_y * lax.axis_size("row")
    wave_x, wave_y = positions(
        (block_x, block_y),
        lax.axis_index("col") * block_x,
        lax.axis_index("row") * block_y,
        length,
    )
    damping, weight_a, weight_b, weight_c = section_weights(wave_x, wave_y, length)[:4]
    linear = (
        damping * start_field
        + weight_a * start_term
        + 2.0 * weight_b * (first_term + second_term)
    )
    linear, weight_c = lax.optimization_barrier((linear, weight_c))
    section_term = jnp.stack([nonlinear(section_field[m], length) for m in range(members)])
    return linear + weight_c * section_term


def solution(mesh):
    return jax.shard_map(
        per_device,
        mesh=mesh,
        in_specs=(
            P(None, None, "col", "row"),
            P(None, None, "col", "row"),
            P(None, None, "col", "row"),
            P(None, None, "col", "row"),
            P(None, None, "col", "row"),
        ),
        out_specs=P(None, None, "col", "row"),
        check_vma=False,
    )
```
